32 devices in a mesh: dp: 1 (over z), ri: 4 (over y), co: 4 (over x), ro: 2 (over core).
Axes of the slice: x: 4, y: 4, z: 1, core: 2. Of those that a mesh axis runs over, the one named last changes fastest.
The devices are a block of a 4x4x8 slice.
Arguments:
- a_mat: bfloat16 [2048, 24576], P(('dp', 'ri', 'ro'), 'co')
- b_mat: bfloat16 [24576, 16384], P(('dp', 'ri', 'ro'), 'co')
Outputs:
- output: bfloat16 [2048, 16384], P(('dp', 'ri', 'ro'), 'co')
All inputs are finite; a program needn't handle non-finite values.
Results may differ from the reference program's by a relative error of at most 0.001.
Values are sent between devices in bfloat16 or wider.
A program may use at most 768 MiB of HBM per device.

```python
import jax
import jax.numpy as jnp

M_ROWS = 2048
N_COLS = 16384
K_DEPTH = 24576


def setup_inputs(seed: int = 0, part: int = 0) -> dict:
    base_key = jax.random.fold_in(jax.random.key(seed), part)
    key_a, key_b = jax.random.split(base_key)
    left_mat = jax.random.normal(key_a, (M_ROWS, K_DEPTH), jnp.float32)
    right_mat = jax.random.normal(key_b, (K_DEPTH, N_COLS), jnp.float32) * (K_DEPTH ** -0.5)
    return {"a_mat": left_mat.astype(jnp.bfloat16), "b_mat": right_mat.astype(jnp.bfloat16)}


def reference(a_mat, b_mat):
    product = jnp.dot(a_mat, b_mat, preferred_element_type=jnp.float32)
    return product.astype(jnp.bfloat16)
```

```python
import functools

import jax
import jax.numpy as jnp
from jax import lax
from jax.experimental import pallas as pl
from jax.experimental.pallas import tpu as pltpu
from jax.sharding import PartitionSpec as P

MESH = pl.DeviceIdType.MESH
HALVES = 2
WIDTH = 512


def kernel(n, a_ref, b_ref, c_ref, b_far, a_all, b_panel, far_out, far_in, near_out, near_in, own, result,
           a1_send, a1_recv, a2_send, a2_recv, local_sem, b_send, b_recv, load_sem,
           far_send, far_recv, near_send, near_recv, result_sem):
    y, x, core = lax.axis_index("ri"), lax.axis_index("co"), lax.axis_index("ro")
    rows, depth = a_ref.shape
    part = depth // n
    half_k = b_ref.shape[0]
    panels = b_ref.shape[1] // WIDTH
    piece = rows // HALVES
    diagonal = x == y

    def wrap(v):
        return lax.rem(v, n)

    def slot_of(off):
        return off // 2 + 2 * (1 - off % 2)

    def cols(q):
        return pl.ds(pl.multiple_of(q * part, 128), part)

    def panel_cols(p):
        return pl.ds(pl.multiple_of(p * WIDTH, 128), WIDTH)

    def lines(h):
        return pl.ds(h * piece, piece)

    def order(i):
        return i // 2 + (panels // 2) * lax.rem(i, 2)

    bar = pltpu.get_barrier_semaphore()

    def greet(**to):
        pl.semaphore_signal(bar, 1, device_id=to, device_id_type=MESH)

    for off in range(1, n):
        greet(ri=wrap(y + off), co=y)
    @pl.when(jnp.logical_not(diagonal))
    def _():
        greet(ri=y, co=y)
    for delta in range(1, n):
        greet(co=wrap(x + delta))
    greet(ri=wrap(y + 1))
    greet(ri=wrap(y + n - 1))
    greet(ro=1 - core)
    @pl.when(diagonal)
    def _():
        pl.semaphore_wait(bar, 2 * n + 1)
    @pl.when(jnp.logical_not(diagonal))
    def _():
        pl.semaphore_wait(bar, 2 * n + 2)

    my_slot = slot_of(wrap(y - x + n))

    def a1_copy(h, dq, slot):
        q = wrap(x + dq)
        return pltpu.make_async_remote_copy(
            a_ref.at[lines(h), cols(q)], a_all.at[slot, lines(h), cols(q)],
            a1_send.at[h, dq], a1_recv.at[slot, h], device_id={"ri": x, "co": q}, device_id_type=MESH)

    def a1_local(h):
        return pltpu.make_async_copy(a_ref.at[lines(h), cols(x)], a_all.at[2, lines(h), cols(x)], local_sem.at[h])

    for h in range(HALVES):
        @pl.when(diagonal)
        def _():
            a1_local(h).start()
        @pl.when(jnp.logical_not(diagonal))
        def _():
            a1_copy(h, 0, my_slot).start()
        for dq in (1, 3, 2):
            a1_copy(h, dq, my_slot).start()

    def b_copy(p):
        return pltpu.make_async_remote_copy(
            b_ref.at[:, panel_cols(p)], b_far.at[:, panel_cols(p)], b_send.at[p], b_recv.at[p],
            device_id={"ro": 1 - core}, device_id_type=MESH)

    for i in range(panels):
        b_copy(order(jnp.int32(i))).start()

    def near_load(p, s):
        return pltpu.make_async_copy(
            b_ref.at[:, panel_cols(p)], b_panel.at[s, pl.ds(pl.multiple_of(core * half_k, 128), half_k), :], load_sem.at[0, s])

    def far_load(p, s):
        return pltpu.make_async_copy(
            b_far.at[:, panel_cols(p)], b_panel.at[s, pl.ds(pl.multiple_of((1 - core) * half_k, 128), half_k), :], load_sem.at[1, s])

    near_load(0, 0).start()

    def a2_copy(slot, h, delta):
        return pltpu.make_async_remote_copy(
            a_all.at[slot, lines(h), cols(x)], a_all.at[slot, lines(h), cols(x)],
            a2_send.at[slot, h, delta - 1], a2_recv.at[slot, h, delta - 1],
            device_id={"co": wrap(x + delta)}, device_id_type=MESH)

    for slot, h in [(3, h) for h in range(HALVES)] + [(s, h) for h in range(HALVES) for s in (0, 1)] + [(2, h) for h in range(HALVES)]:
        if slot == 2:
            @pl.when(diagonal)
            def _():
                a1_local(h).wait()
            @pl.when(jnp.logical_not(diagonal))
            def _():
                a1_copy(h, 0, slot).wait_recv()
        else:
            a1_copy(h, 0, slot).wait_recv()
        for delta in (1, 3, 2):
            a2_copy(slot, h, delta).start()

    b_copy(0).wait_recv()
    far_load(0, 0).start()

    def far_copy(h, p):
        return pltpu.make_async_remote_copy(
            far_out.at[h, p], far_in.at[h, p], far_send.at[h, p], far_recv.at[h, p],
            device_id={"ri": wrap(y + n - 1 - 2 * (p // (panels // 2)) + n)}, device_id_type=MESH)

    def near_copy(j, h, p):
        return pltpu.make_async_remote_copy(
            near_out.at[j, h, p], near_in.at[j, h, p], near_send.at[j, h, p], near_recv.at[j, h, p],
            device_id={"ri": wrap(y + 1 + (n - 2) * j)}, device_id_type=MESH)

    def send(kind, h, p):
        if kind == "far":
            far_copy(h, p).start()
        elif kind == "near":
            near_copy(0, h, p).start()
            near_copy(1, h, p).start()

    units = [("far", h) for h in range(HALVES)] + [("near", h) for h in range(HALVES)] + [("own", 0)]
    for u, (kind, h) in enumerate(units):
        waits = {"far": [(3, h)], "near": [(0, h), (1, h)], "own": [(2, g) for g in range(HALVES)]}[kind]
        for slot, g in waits:
            for delta in (1, 3, 2):
                a2_copy(slot, g, delta).wait_recv()

        def step(i, _, u=u, kind=kind, h=h):
            p, s = order(i), lax.rem(i, 2)
            if u + 1 < len(units):
                more = i >= 0
            else:
                more = i + 1 < panels
            p1 = order(lax.rem(i + 1, panels))

            @pl.when(more)
            def _():
                near_load(p1, 1 - s).start()
                if u == 0:
                    @pl.when(i + 1 < panels)
                    def _():
                        b_copy(p1).wait_recv()
                far_load(p1, 1 - s).start()
            near_load(p, s).wait()
            far_load(p, s).wait()
            if kind == "near":
                lhs = a_all[0:2, h * piece:(h + 1) * piece].reshape(2 * piece, depth)
            elif kind == "far":
                lhs = a_all[3, h * piece:(h + 1) * piece]
            else:
                lhs = a_all[2]
            value = jnp.dot(lhs, b_panel[s], preferred_element_type=jnp.float32)
            @pl.when(i > 0)
            def _():
                send(kind, h, order(i - 1))
            if u > 0:
                @pl.when(i == 0)
                def _():
                    send(*units[u - 1], panels - 1)
            if kind == "far":
                far_out[h, p] = value
            elif kind == "near":
                near_out[0, h, p] = value[:piece]
                near_out[1, h, p] = value[piece:]
                far_copy(h, p).wait_recv()
                j = 1 - p // (panels // 2)
                near_out[j, h, p] += far_in[h, p]
            else:
                own[:, panel_cols(p)] = value
            return 0

        lax.fori_loop(0, panels, step, 0)

    def result_copy(p):
        return pltpu.make_async_copy(result.at[:, panel_cols(p)], c_ref.at[:, panel_cols(p)], result_sem.at[p])

    def finish(i, _):
        p = order(i)
        for h in range(HALVES):
            near_copy(0, h, p).wait_recv()
            near_copy(1, h, p).wait_recv()
            total = own[h * piece:(h + 1) * piece, panel_cols(p)] + near_in[0, h, p] + near_in[1, h, p]
            result[h * piece:(h + 1) * piece, panel_cols(p)] = total.astype(jnp.bfloat16)
        @pl.when(i > 0)
        def _():
            result_copy(order(i - 1)).start()
        return 0

    lax.fori_loop(0, panels, finish, 0)

    for h in range(HALVES):
        @pl.when(jnp.logical_not(diagonal))
        def _():
            a1_copy(h, 0, my_slot).wait_send()
        for dq in (1, 3, 2):
            a1_copy(h, dq, my_slot).wait_send()
        for slot in range(n):
            for delta in (1, 3, 2):
                a2_copy(slot, h, delta).wait_send()

    def drain(p, _):
        b_copy(p).wait_send()
        for h in range(HALVES):
            far_copy(h, p).wait_send()
            near_copy(0, h, p).wait_send()
            near_copy(1, h, p).wait_send()
        return 0

    lax.fori_loop(0, panels, drain, 0)
    result_copy(panels - 1).start()

    def drain_result(p, _):
        result_copy(p).wait()
        return 0

    lax.fori_loop(0, panels, drain_result, 0)


def solution(mesh):
    n = mesh.shape["ri"]
    spec = P(("dp", "ri", "ro"), "co")

    def block(a, b):
        rows, depth = a.shape
        half_k, width = b.shape
        panels, piece = width // WIDTH, rows // HALVES
        f32, bf16 = jnp.float32, jnp.bfloat16
        dma = pltpu.SemaphoreType.DMA
        hbm = pl.BlockSpec(memory_space=pl.ANY)
        c, _ = pl.pallas_call(
            functools.partial(kernel, n),
            out_shape=(jax.ShapeDtypeStruct((rows, width), bf16), jax.ShapeDtypeStruct((half_k, width), bf16)),
            in_specs=[hbm, hbm],
            out_specs=(hbm, hbm),
            scratch_shapes=[
                pltpu.VMEM((n, rows, depth), bf16),
                pltpu.VMEM((2, 2 * half_k, WIDTH), bf16),
                pltpu.VMEM((HALVES, panels, piece, WIDTH), f32),
                pltpu.VMEM((HALVES, panels, piece, WIDTH), f32),
                pltpu.VMEM((2, HALVES, panels, piece, WIDTH), f32),
                pltpu.VMEM((2, HALVES, panels, piece, WIDTH), f32),
                pltpu.VMEM((rows, width), f32),
                pltpu.VMEM((rows, width), bf16),
                dma((HALVES, n)), dma((n, HALVES)), dma((n, HALVES, n - 1)), dma((n, HALVES, n - 1)), dma((HALVES,)),
                dma((panels,)), dma((panels,)), dma((2, 2)),
                dma((HALVES, panels)), dma((HALVES, panels)), dma((2, HALVES, panels)), dma((2, HALVES, panels)),
                dma((panels,)),
            ],
            compiler_params=pltpu.CompilerParams(
                collective_id=0, has_side_effects=True, vmem_limit_bytes=63 * 2**20),
        )(a, b)
        return c

    return jax.shard_map(block, mesh=mesh, in_specs=(spec, spec), out_specs=spec, check_vma=False)
```

```python
import functools

import jax
import jax.numpy as jnp
from jax import lax
from jax.experimental import pallas as pl
from jax.experimental.pallas import tpu as pltpu
from jax.sharding import PartitionSpec as P

MESH = pl.DeviceIdType.MESH
HALVES = 2
WIDTH = 512


def kernel(n, a_ref, b_ref, c_ref, b_far, a_all, b_panel, far_out, far_in, near_out, near_in, own, result, a_way,
           a0_send, a0_recv, a1_send, a1_recv, a2_send, a2_recv, local_sem, b_send, b_recv, load_sem,
           far_send, far_recv, near_send, near_recv, result_sem):
    y, x, core = lax.axis_index("ri"), lax.axis_index("co"), lax.axis_index("ro")
    rows, depth = a_ref.shape
    part = depth // n
    half_k = b_ref.shape[0]
    panels = b_ref.shape[1] // WIDTH
    piece = rows // HALVES
    diagonal = x == y

    def wrap(v):
        return lax.rem(v, n)

    def slot_of(off):
        return off // 2 + 2 * (1 - off % 2)

    def cols(q):
        return pl.ds(pl.multiple_of(q * part, 128), part)

    def panel_cols(p):
        return pl.ds(pl.multiple_of(p * WIDTH, 128), WIDTH)

    def lines(h):
        return pl.ds(h * piece, piece)

    def order(i):
        return i // 2 + (panels // 2) * lax.rem(i, 2)

    bar = pltpu.get_barrier_semaphore()

    def greet(**to):
        pl.semaphore_signal(bar, 1, device_id=to, device_id_type=MESH)

    for delta in range(1, n):
        greet(co=wrap(x + delta))
        greet(ri=wrap(y + delta))
    greet(ro=1 - core)
    pl.semaphore_wait(bar, 2 * n - 1)

    def a0_copy(h, delta, direct):
        q = wrap(x + delta)
        dst = a_all.at[2, lines(h), cols(q)] if direct else a_way.at[delta - 1, h]
        return pltpu.make_async_remote_copy(
            a_ref.at[lines(h), cols(q)], dst, a0_send.at[h, delta - 1], a0_recv.at[h, delta - 1],
            device_id={"co": q}, device_id_type=MESH)

    def a_local(h):
        return pltpu.make_async_copy(a_ref.at[lines(h), cols(x)], a_all.at[2, lines(h), cols(x)], local_sem.at[h])

    for h in range(HALVES):
        @pl.when(diagonal)
        def _():
            a_local(h).start()
            for delta in (1, 3, 2):
                a0_copy(h, delta, True).start()
        @pl.when(jnp.logical_not(diagonal))
        def _():
            for delta in (1, 3, 2):
                a0_copy(h, delta, False).start()

    def a1_copy(h, off, src):
        slot = slot_of(off)
        return pltpu.make_async_remote_copy(
            src, a_all.at[slot, lines(h), cols(x)], a1_send.at[h, off - 1], a1_recv.at[slot, h],
            device_id={"ri": wrap(y - off + n)}, device_id_type=MESH)

    def a1_start(h, off):
        delta = wrap(x - y + off + n)
        @pl.when(delta == 0)
        def _():
            a1_copy(h, off, a_ref.at[lines(h), cols(x)]).start()
        for e in range(1, n):
            @pl.when(delta == e)
            def _():
                a0_copy(h, e, False).wait_recv()
                a1_copy(h, off, a_way.at[e - 1, h]).start()

    def b_copy(p):
        return pltpu.make_async_remote_copy(
            b_ref.at[:, panel_cols(p)], b_far.at[:, panel_cols(p)], b_send.at[p], b_recv.at[p],
            device_id={"ro": 1 - core}, device_id_type=MESH)

    for i in range(panels):
        b_copy(order(jnp.int32(i))).start()

    def near_load(p, s):
        return pltpu.make_async_copy(
            b_ref.at[:, panel_cols(p)], b_panel.at[s, pl.ds(pl.multiple_of(core * half_k, 128), half_k), :], load_sem.at[0, s])

    def far_load(p, s):
        return pltpu.make_async_copy(
            b_far.at[:, panel_cols(p)], b_panel.at[s, pl.ds(pl.multiple_of((1 - core) * half_k, 128), half_k), :], load_sem.at[1, s])

    near_load(0, 0).start()

    def a2_copy(slot, h, kind):
        if kind < 2 or kind == 4:
            view = a_all.at[slot, lines(h), cols(x)]
        else:
            view = a_all.at[slot, pl.ds(h * piece + (kind - 2) * (piece // 2), piece // 2), cols(wrap(x + (n - 1, 1)[kind - 2]))]
        return pltpu.make_async_remote_copy(
            view, view, a2_send.at[slot, h, kind], a2_recv.at[slot, h, kind],
            device_id={"co": wrap(x + (1, n - 1, 1, n - 1, 2)[kind])}, device_id_type=MESH)

    def a2_start(slot, h):
        if slot == 2:
            @pl.when(diagonal)
            def _():
                a_local(h).wait()
            for e in range(1, n):
                @pl.when(wrap(x - y + n) == e)
                def _():
                    a0_copy(h, e, False).wait_recv()
        else:
            a1_copy(h, (2 * slot + 1 if slot < 2 else 2), a_way.at[0, h]).wait_recv()
        a2_copy(slot, h, 0).start()
        a2_copy(slot, h, 1).start()
        if slot != 3:
            a2_copy(slot, h, 4).start()

    def relay(slot, h):
        for kind in (0, 1):
            a2_copy(slot, h, kind).wait_recv()
            a2_copy(slot, h, kind + 2).start()

    for off in (2, 1, 3):
        a1_start(0, off)
    a2_start(3, 0)
    for off in (2, 1, 3):
        a1_start(1, off)
    relay(3, 0)
    a2_start(3, 1)

    hooks = {
        (0, 1): [lambda: relay(3, 1)],
        (0, 2): [lambda: a2_start(0, 0), lambda: a2_start(1, 0)],
        (0, 4): [lambda: a2_start(0, 1), lambda: a2_start(1, 1)],
        (1, 1): [lambda: a2_start(2, 0), lambda: a2_start(2, 1)],
    }

    b_copy(0).wait_recv()
    far_load(0, 0).start()

    def far_copy(h, p):
        return pltpu.make_async_remote_copy(
            far_out.at[h, p], far_in.at[h, p], far_send.at[h, p], far_recv.at[h, p],
            device_id={"ri": wrap(y + n - 1 - 2 * (p // (panels // 2)) + n)}, device_id_type=MESH)

    def near_copy(j, h, p):
        return pltpu.make_async_remote_copy(
            near_out.at[j, h, p], near_in.at[j, h, p], near_send.at[j, h, p], near_recv.at[j, h, p],
            device_id={"ri": wrap(y + 1 + (n - 2) * j)}, device_id_type=MESH)

    def send(kind, h, p):
        if kind == "far":
            far_copy(h, p).start()
        elif kind == "near":
            near_copy(0, h, p).start()
            near_copy(1, h, p).start()

    units = [("far", h) for h in range(HALVES)] + [("near", h) for h in range(HALVES)] + [("own", 0)]
    for u, (kind, h) in enumerate(units):
        waits = {"far": [(3, h)], "near": [(0, h), (1, h)], "own": [(2, g) for g in range(HALVES)]}[kind]
        for slot, g in waits:
            for k in (2, 3) if slot == 3 else (0, 1, 4):
                a2_copy(slot, g, k).wait_recv()

        def step(i, _, u=u, kind=kind, h=h):
            p, s = order(i), lax.rem(i, 2)
            if u + 1 < len(units):
                more = i >= 0
            else:
                more = i + 1 < panels
            p1 = order(lax.rem(i + 1, panels))

            @pl.when(more)
            def _():
                near_load(p1, 1 - s).start()
                if u == 0:
                    @pl.when(i + 1 < panels)
                    def _():
                        b_copy(p1).wait_recv()
                far_load(p1, 1 - s).start()
            near_load(p, s).wait()
            far_load(p, s).wait()
            if kind == "near":
                lhs = a_all[0:2, h * piece:(h + 1) * piece].reshape(2 * piece, depth)
            elif kind == "far":
                lhs = a_all[3, h * piece:(h + 1) * piece]
            else:
                lhs = a_all[2]
            value = jnp.dot(lhs, b_panel[s], preferred_element_type=jnp.float32)
            @pl.when(i > 0)
            def _():
                send(kind, h, order(i - 1))
            if u > 0:
                @pl.when(i == 0)
                def _():
                    send(*units[u - 1], panels - 1)
            if kind == "far":
                far_out[h, p] = value
            elif kind == "near":
                near_out[0, h, p] = value[:piece]
                near_out[1, h, p] = value[piece:]
                far_copy(h, p).wait_recv()
                j = 1 - p // (panels // 2)
                near_out[j, h, p] += far_in[h, p]
            else:
                own[:, panel_cols(p)] = value
            for (w, at), work in hooks.items():
                if w == u:
                    @pl.when(i == at)
                    def _(work=work):
                        for do in work:
                            do()
            return 0

        lax.fori_loop(0, panels, step, 0)

    def result_copy(p):
        return pltpu.make_async_copy(result.at[:, panel_cols(p)], c_ref.at[:, panel_cols(p)], result_sem.at[p])

    def finish(i, _):
        p = order(i)
        for h in range(HALVES):
            near_copy(0, h, p).wait_recv()
            near_copy(1, h, p).wait_recv()
            total = own[h * piece:(h + 1) * piece, panel_cols(p)] + near_in[0, h, p] + near_in[1, h, p]
            result[h * piece:(h + 1) * piece, panel_cols(p)] = total.astype(jnp.bfloat16)
        @pl.when(i > 0)
        def _():
            result_copy(order(i - 1)).start()
        return 0

    lax.fori_loop(0, panels, finish, 0)

    for h in range(HALVES):
        for delta in range(1, n):
            a0_copy(h, delta, False).wait_send()
            a1_copy(h, delta, a_way.at[0, h]).wait_send()
        for slot in range(n):
            for kind in (0, 1, 2, 3) if slot == 3 else (0, 1, 4):
                a2_copy(slot, h, kind).wait_send()

    def drain(p, _):
        b_copy(p).wait_send()
        for h in range(HALVES):
            far_copy(h, p).wait_send()
            near_copy(0, h, p).wait_send()
            near_copy(1, h, p).wait_send()
        return 0

    lax.fori_loop(0, panels, drain, 0)
    result_copy(panels - 1).start()

    def drain_result(p, _):
        result_copy(p).wait()
        return 0

    lax.fori_loop(0, panels, drain_result, 0)


def solution(mesh):
    n = mesh.shape["ri"]
    spec = P(("dp", "ri", "ro"), "co")

    def block(a, b):
        rows, depth = a.shape
        half_k, width = b.shape
        panels, piece = width // WIDTH, rows // HALVES
        f32, bf16 = jnp.float32, jnp.bfloat16
        dma = pltpu.SemaphoreType.DMA
        hbm = pl.BlockSpec(memory_space=pl.ANY)
        c, _ = pl.pallas_call(
            functools.partial(kernel, n),
            out_shape=(jax.ShapeDtypeStruct((rows, width), bf16), jax.ShapeDtypeStruct((half_k, width), bf16)),
            in_specs=[hbm, hbm],
            out_specs=(hbm, hbm),
            scratch_shapes=[
                pltpu.VMEM((n, rows, depth), bf16),
                pltpu.VMEM((2, 2 * half_k, WIDTH), bf16),
                pltpu.VMEM((HALVES, panels, piece, WIDTH), f32),
                pltpu.VMEM((HALVES, panels, piece, WIDTH), f32),
                pltpu.VMEM((2, HALVES, panels, piece, WIDTH), f32),
                pltpu.VMEM((2, HALVES, panels, piece, WIDTH), f32),
                pltpu.VMEM((rows, width), f32),
                pltpu.VMEM((rows, width), bf16),
                pltpu.VMEM((n - 1, HALVES, piece, depth // n), bf16),
                dma((HALVES, n - 1)), dma((HALVES, n - 1)), dma((HALVES, n - 1)), dma((n, HALVES)), dma((n, HALVES, 5)), dma((n, HALVES, 5)), dma((HALVES,)),
                dma((panels,)), dma((panels,)), dma((2, 2)),
                dma((HALVES, panels)), dma((HALVES, panels)), dma((2, HALVES, panels)), dma((2, HALVES, panels)),
                dma((panels,)),
            ],
            compiler_params=pltpu.CompilerParams(
                collective_id=0, has_side_effects=True, vmem_limit_bytes=63 * 2**20),
        )(a, b)
        return c

    return jax.shard_map(block, mesh=mesh, in_specs=(spec, spec), out_specs=spec, check_vma=False)
```

```python
import functools

import jax
import jax.numpy as jnp
from jax import lax
from jax.experimental import pallas as pl
from jax.experimental.pallas import tpu as pltpu
from jax.sharding import PartitionSpec as P

MESH = pl.DeviceIdType.MESH
HALVES = 2
PIECES = 4
WIDTH = 512


def kernel(n, a_ref, b_ref, c_ref, b_far, a_all, b_panel, far_out, far_in, near_out, near_in, own, result, a_way,
           a0_send, a0_recv, a1_send, a1_recv, a2_send, a2_recv, local_sem, b_send, b_recv, load_sem,
           far_send, far_recv, near_send, near_recv, result_sem):
    y, x, core = lax.axis_index("ri"), lax.axis_index("co"), lax.axis_index("ro")
    rows, depth = a_ref.shape
    part = depth // n
    half_k = b_ref.shape[0]
    panels = b_ref.shape[1] // WIDTH
    piece = rows // HALVES
    diagonal = x == y

    def wrap(v):
        return lax.rem(v, n)

    def slot_of(off):
        return off // 2 + 2 * (1 - off % 2)

    def cols(q):
        return pl.ds(pl.multiple_of(q * part, 128), part)

    def panel_cols(p):
        return pl.ds(pl.multiple_of(p * WIDTH, 128), WIDTH)

    def lines(h):
        return pl.ds(h * piece, piece)

    def bits(p):
        return pl.ds(p * (rows // PIECES), rows // PIECES)

    per_half = PIECES // HALVES

    def order(i):
        return i // 2 + (panels // 2) * lax.rem(i, 2)

    bar = pltpu.get_barrier_semaphore()

    def greet(**to):
        pl.semaphore_signal(bar, 1, device_id=to, device_id_type=MESH)

    for delta in range(1, n):
        greet(co=wrap(x + delta))
        greet(ri=wrap(y + delta))
    greet(ro=1 - core)
    pl.semaphore_wait(bar, 2 * n - 1)

    def a0_copy(p, delta, direct):
        q = wrap(x + delta)
        dst = a_all.at[2, bits(p), cols(q)] if direct else a_way.at[delta - 1, p]
        return pltpu.make_async_remote_copy(
            a_ref.at[bits(p), cols(q)], dst, a0_send.at[p, delta - 1], a0_recv.at[p, delta - 1],
            device_id={"co": q}, device_id_type=MESH)

    def a_local():
        return pltpu.make_async_copy(a_ref.at[:, cols(x)], a_all.at[2, :, cols(x)], local_sem.at[0])

    def a0_start(p):
        @pl.when(diagonal)
        def _():
            for delta in (1, 3, 2):
                a0_copy(p, delta, True).start()
        @pl.when(jnp.logical_not(diagonal))
        def _():
            for delta in (1, 3, 2):
                a0_copy(p, delta, False).start()

    for p in range(PIECES):
        a0_start(p)
    @pl.when(diagonal)
    def _():
        a_local().start()

    def a1_copy(p, off, src):
        slot = slot_of(off)
        return pltpu.make_async_remote_copy(
            src, a_all.at[slot, bits(p), cols(x)], a1_send.at[p, off - 1], a1_recv.at[slot, p],
            device_id={"ri": wrap(y - off + n)}, device_id_type=MESH)

    def a1_start(p, off):
        delta = wrap(x - y + off + n)
        @pl.when(delta == 0)
        def _():
            a1_copy(p, off, a_ref.at[bits(p), cols(x)]).start()
        for e in range(1, n):
            @pl.when(delta == e)
            def _():
                a0_copy(p, e, False).wait_recv()
                a1_copy(p, off, a_way.at[e - 1, p]).start()

    def b_copy(p):
        return pltpu.make_async_remote_copy(
            b_ref.at[:, panel_cols(p)], b_far.at[:, panel_cols(p)], b_send.at[p], b_recv.at[p],
            device_id={"ro": 1 - core}, device_id_type=MESH)

    for i in range(panels):
        b_copy(order(jnp.int32(i))).start()

    def near_load(p, s):
        return pltpu.make_async_copy(
            b_ref.at[:, panel_cols(p)], b_panel.at[s, pl.ds(pl.multiple_of(core * half_k, 128), half_k), :], load_sem.at[0, s])

    def far_load(p, s):
        return pltpu.make_async_copy(
            b_far.at[:, panel_cols(p)], b_panel.at[s, pl.ds(pl.multiple_of((1 - core) * half_k, 128), half_k), :], load_sem.at[1, s])

    near_load(0, 0).start()

    def a2_copy(slot, h, kind):
        if kind < 2 or kind == 4:
            view = a_all.at[slot, lines(h), cols(x)]
        else:
            view = a_all.at[slot, pl.ds(h * piece + (kind - 2) * (piece // 2), piece // 2), cols(wrap(x + (n - 1, 1)[kind - 2]))]
        return pltpu.make_async_remote_copy(
            view, view, a2_send.at[slot, h, kind], a2_recv.at[slot, h, kind],
            device_id={"co": wrap(x + (1, n - 1, 1, n - 1, 2)[kind])}, device_id_type=MESH)

    def passed_on(slot, h):
        return slot == 3 or (slot < 2 and h == 0)

    def a2_start(slot, h):
        for p in range(h * per_half, (h + 1) * per_half):
            if slot == 2:
                for e in range(1, n):
                    @pl.when(wrap(x - y + n) == e)
                    def _():
                        a0_copy(p, e, False).wait_recv()
            else:
                a1_copy(p, (2 * slot + 1 if slot < 2 else 2), a_way.at[0, p]).wait_recv()
        if slot == 2 and h == 0:
            @pl.when(diagonal)
            def _():
                a_local().wait()
        a2_copy(slot, h, 0).start()
        a2_copy(slot, h, 1).start()
        if not passed_on(slot, h):
            a2_copy(slot, h, 4).start()

    def relay(slot, h):
        for kind in (0, 1):
            a2_copy(slot, h, kind).wait_recv()
            a2_copy(slot, h, kind + 2).start()

    for h in range(HALVES):
        for p in range(h * per_half, (h + 1) * per_half):
            for off in (2, 1, 3):
                a1_start(p, off)
        if h == 0:
            a2_start(3, 0)
    relay(3, 0)
    a2_start(3, 1)

    hooks = {
        (0, 3): [lambda: relay(3, 1), lambda: a2_start(0, 0), lambda: a2_start(1, 0)],
        (1, 3): [lambda: relay(0, 0)],
        (1, 6): [lambda: relay(1, 0)],
        (1, 7): [lambda: a2_start(0, 1), lambda: a2_start(1, 1), lambda: a2_start(2, 0), lambda: a2_start(2, 1)],
    }

    b_copy(0).wait_recv()
    far_load(0, 0).start()

    def far_copy(h, p):
        return pltpu.make_async_remote_copy(
            far_out.at[h, p], far_in.at[h, p], far_send.at[h, p], far_recv.at[h, p],
            device_id={"ri": wrap(y + n - 1 - 2 * (p // (panels // 2)) + n)}, device_id_type=MESH)

    def near_copy(j, h, p):
        return pltpu.make_async_remote_copy(
            near_out.at[j, h, p], near_in.at[j, h, p], near_send.at[j, h, p], near_recv.at[j, h, p],
            device_id={"ri": wrap(y + 1 + (n - 2) * j)}, device_id_type=MESH)

    def send(kind, h, p):
        if kind == "far":
            far_copy(h, p).start()
        elif kind == "near":
            near_copy(0, h, p).start()
            near_copy(1, h, p).start()

    units = [("far", h) for h in range(HALVES)] + [("near", h) for h in range(HALVES)] + [("own", 0)]
    for u, (kind, h) in enumerate(units):
        waits = {"far": [(3, h)], "near": [(0, h), (1, h)], "own": [(2, g) for g in range(HALVES)]}[kind]
        for slot, g in waits:
            for k in (2, 3) if passed_on(slot, g) else (0, 1, 4):
                a2_copy(slot, g, k).wait_recv()

        def step(i, _, u=u, kind=kind, h=h):
            p, s = order(i), lax.rem(i, 2)
            if u + 1 < len(units):
                more = i >= 0
            else:
                more = i + 1 < panels
            p1 = order(lax.rem(i + 1, panels))

            @pl.when(more)
            def _():
                near_load(p1, 1 - s).start()
                if u == 0:
                    @pl.when(i + 1 < panels)
                    def _():
                        b_copy(p1).wait_recv()
                far_load(p1, 1 - s).start()
            near_load(p, s).wait()
            far_load(p, s).wait()
            if kind == "near":
                lhs = a_all[0:2, h * piece:(h + 1) * piece].reshape(2 * piece, depth)
            elif kind == "far":
                lhs = a_all[3, h * piece:(h + 1) * piece]
            else:
                lhs = a_all[2]
            value = jnp.dot(lhs, b_panel[s], preferred_element_type=jnp.float32)
            @pl.when(i > 0)
            def _():
                send(kind, h, order(i - 1))
            if u > 0:
                @pl.when(i == 0)
                def _():
                    send(*units[u - 1], panels - 1)
            if kind == "far":
                far_out[h, p] = value
            elif kind == "near":
                near_out[0, h, p] = value[:piece]
                near_out[1, h, p] = value[piece:]
                far_copy(h, p).wait_recv()
                j = 1 - p // (panels // 2)
                near_out[j, h, p] += far_in[h, p]
            else:
                own[:, panel_cols(p)] = value
            for (w, at), work in hooks.items():
                if w == u:
                    @pl.when(i == at)
                    def _(work=work):
                        for do in work:
                            do()
            return 0

        lax.fori_loop(0, panels, step, 0)

    def result_copy(p):
        return pltpu.make_async_copy(result.at[:, panel_cols(p)], c_ref.at[:, panel_cols(p)], result_sem.at[p])

    def finish(i, _):
        p = order(i)
        for h in range(HALVES):
            near_copy(0, h, p).wait_recv()
            near_copy(1, h, p).wait_recv()
            total = own[h * piece:(h + 1) * piece, panel_cols(p)] + near_in[0, h, p] + near_in[1, h, p]
            result[h * piece:(h + 1) * piece, panel_cols(p)] = total.astype(jnp.bfloat16)
        @pl.when(i > 0)
        def _():
            result_copy(order(i - 1)).start()
        return 0

    lax.fori_loop(0, panels, finish, 0)

    for p in range(PIECES):
        for delta in range(1, n):
            a0_copy(p, delta, False).wait_send()
            a1_copy(p, delta, a_way.at[0, p]).wait_send()
    for h in range(HALVES):
        for slot in range(n):
            for kind in (0, 1, 2, 3) if passed_on(slot, h) else (0, 1, 4):
                a2_copy(slot, h, kind).wait_send()

    def drain(p, _):
        b_copy(p).wait_send()
        for h in range(HALVES):
            far_copy(h, p).wait_send()
            near_copy(0, h, p).wait_send()
            near_copy(1, h, p).wait_send()
        return 0

    lax.fori_loop(0, panels, drain, 0)
    result_copy(panels - 1).start()

    def drain_result(p, _):
        result_copy(p).wait()
        return 0

    lax.fori_loop(0, panels, drain_result, 0)


def solution(mesh):
    n = mesh.shape["ri"]
    spec = P(("dp", "ri", "ro"), "co")

    def block(a, b):
        rows, depth = a.shape
        half_k, width = b.shape
        panels, piece = width // WIDTH, rows // HALVES
        f32, bf16 = jnp.float32, jnp.bfloat16
        dma = pltpu.SemaphoreType.DMA
        hbm = pl.BlockSpec(memory_space=pl.ANY)
        c, _ = pl.pallas_call(
            functools.partial(kernel, n),
            out_shape=(jax.ShapeDtypeStruct((rows, width), bf16), jax.ShapeDtypeStruct((half_k, width), bf16)),
            in_specs=[hbm, hbm],
            out_specs=(hbm, hbm),
            scratch_shapes=[
                pltpu.VMEM((n, rows, depth), bf16),
                pltpu.VMEM((2, 2 * half_k, WIDTH), bf16),
                pltpu.VMEM((HALVES, panels, piece, WIDTH), f32),
                pltpu.VMEM((HALVES, panels, piece, WIDTH), f32),
                pltpu.VMEM((2, HALVES, panels, piece, WIDTH), f32),
                pltpu.VMEM((2, HALVES, panels, piece, WIDTH), f32),
                pltpu.VMEM((rows, width), f32),
                pltpu.VMEM((rows, width), bf16),
                pltpu.VMEM((n - 1, PIECES, rows // PIECES, depth // n), bf16),
                dma((PIECES, n - 1)), dma((PIECES, n - 1)), dma((PIECES, n - 1)), dma((n, PIECES)), dma((n, HALVES, 5)), dma((n, HALVES, 5)), dma((1,)),
                dma((panels,)), dma((panels,)), dma((2, 2)),
                dma((HALVES, panels)), dma((HALVES, panels)), dma((2, HALVES, panels)), dma((2, HALVES, panels)),
                dma((panels,)),
            ],
            compiler_params=pltpu.CompilerParams(
                collective_id=0, has_side_effects=True, vmem_limit_bytes=63 * 2**20),
        )(a, b)
        return c

    return jax.shard_map(block, mesh=mesh, in_specs=(spec, spec), out_specs=spec, check_vma=False)
```
